32 devices in a mesh: dp: 8 (over y, x, core), expert: 4 (over z).
Axes of the slice: x: 2, y: 2, z: 4, core: 2. Of those that a mesh axis runs over, the one named last changes fastest.
Arguments:
- grad_out: bfloat16 [20480, 1024], P(('dp', 'expert')), may hold values from -3 to 3
- hidden_acts: bfloat16 [20480, 384], P(('dp', 'expert')), may hold values from -0.23925781 to 0.23925781
- expert_ids: int32 [20480], P(('dp', 'expert')), may hold values from 0 to 3, as said below
- down_weight: bfloat16 [4, 384, 1024], P('expert'), may hold values from -0.1875 to 0.1875
- error_in: bfloat16 [8, 4, 384, 1024], P('dp', 'expert'), may hold values from -0.8984375 to 0.8984375
- q_prev: float32 [4, 1024, 32], P('expert'), may hold values from -6 to 6
Outputs:
- grad_hidden: bfloat16 [20480, 384], P(('dp', 'expert'))
- left_factor: float32 [4, 384, 32], P('expert')
- right_factor: float32 [4, 1024, 32], P('expert')
- error_out: bfloat16 [8, 4, 384, 1024], P('dp', 'expert')
The draws below stay inside these ranges and needn't reach their ends.
Inputs may be any that keep to these rules, and one draw needn't show every extreme that they name: `expert_ids`: the rows of one device name each expert at most 320 times; in every replica some expert is named exactly 320 times by the rows of every device of that replica.
All inputs are finite; a program needn't handle non-finite values.
Results may differ from the reference program's by a relative error of at most 0.0004.
Values may be sent and summed in bfloat16 or wider, within the bound.
No kernel may reach another device: no remote copies, remote signals or barrier semaphores. Data moves between devices by JAX's collectives and lax.ppermute only.
A program may use at most 64 MiB of HBM per device.

```python
import jax
import jax.numpy as jnp
from jax import lax

D_WIN = 1024
F_WIN = 384
RANK = 32
ROWS_DEV = 640
EXPERTS = 4
CAP = 320
ROWS = 20480
N_DP = 8


def draw_expert_ids(key, part):
    blocks = ROWS // ROWS_DEV
    replicas = blocks // EXPERTS
    slot_count = EXPERTS * CAP
    slot_expert = jnp.arange(slot_count, dtype=jnp.int32) // CAP
    slot_order = jnp.arange(slot_count, dtype=jnp.int32)
    key_list = jax.random.split(jax.random.fold_in(key, 17), 3)
    hot_list = jax.random.randint(key_list[0], (replicas,), 0, EXPERTS)
    popular = jax.random.randint(key_list[1], (replicas, EXPERTS), 1, 9)

    def one_block(block_index, block_key):
        replica = block_index // EXPERTS
        score_key, order_key = jax.random.split(block_key)
        noise_draw = jax.random.randint(score_key, (slot_count,), 0, 32768)
        weights = popular[replica][slot_expert]
        scores = noise_draw * weights * slot_count + slot_order
        scores = jnp.where(slot_expert == hot_list[replica], 2 ** 30 + slot_order, scores)
        _, chosen = lax.top_k(scores, ROWS_DEV)
        picked = slot_expert[chosen]
        return picked[jax.random.permutation(order_key, ROWS_DEV)]
    expert_list = jax.vmap(one_block)(jnp.arange(blocks, dtype=jnp.int32), jax.random.split(key_list[2], blocks))
    return expert_list.reshape(-1).astype(jnp.int32)


def shard_levels(rng, dims, cuts, smallest, top_value):
    gain, own = 1.0, jax.random.fold_in(rng, 6)
    for dim, shards_of in cuts:
        steps = jnp.exp(jax.random.uniform(jax.random.fold_in(own, dim), (shards_of,), jnp.float32, smallest / len(cuts), top_value / len(cuts)))
        gain = gain * jnp.repeat(steps, dims[dim] // shards_of).reshape([-1 if axis == dim else 1 for axis in range(len(dims))])
    return gain


def scatter_about(stream_key, dims, width, reach, pieces=(), kind=jnp.bfloat16):
    drawn = width * jax.random.normal(stream_key, dims, jnp.float32)
    if pieces:
        drawn = drawn * shard_levels(stream_key, dims, pieces, -0.22, 0.18)
    return jnp.clip(drawn, -reach, reach).astype(kind)


def setup_inputs(seed: int = 0) -> dict:
    splits = jax.random.split(jax.random.key(seed), 7)
    return {
        "grad_out": scatter_about(splits[0], (ROWS, D_WIN), 0.5, 3.0, ((0, 32),)),
        "hidden_acts": scatter_about(splits[1], (ROWS, F_WIN), 0.04, 0.23925781, ((0, 32),)),
        "expert_ids": draw_expert_ids(jax.random.fold_in(splits[6], 71), 0),
        "down_weight": scatter_about(splits[3], (EXPERTS, F_WIN, D_WIN), D_WIN ** -0.5, 0.1875, ((0, 4),)),
        "error_in": scatter_about(splits[4], (N_DP, EXPERTS, F_WIN, D_WIN), 0.15, 0.8984375, ((0, 8), (1, 4))),
        "q_prev": scatter_about(splits[5], (EXPERTS, D_WIN, RANK), 1.0, 6.0, ((0, 4),), jnp.float32),
    }


def place_rows(expert_list, count):
    onehot = (expert_list[:, None] == jnp.arange(count, dtype=jnp.int32)[None, :]).astype(jnp.int32)
    ranks = jnp.cumsum(onehot, axis=0) - 1
    return jnp.sum(ranks * onehot, axis=1).astype(jnp.int32)

def reference(grad_out, hidden_acts, expert_ids, down_weight, error_in, q_prev):
    replica_rows = EXPERTS * ROWS_DEV
    weight_full = down_weight.astype(jnp.float32)

    def one_replica(replica):
        start = (replica * replica_rows).astype(jnp.int32)
        grad_rows = lax.dynamic_slice_in_dim(grad_out, start, replica_rows, 0)
        hidden_rows = lax.dynamic_slice_in_dim(hidden_acts, start, replica_rows, 0)
        expert_list = lax.dynamic_slice_in_dim(expert_ids, start, replica_rows, 0).reshape(EXPERTS, ROWS_DEV)
        position = jax.vmap(lambda row_ids: place_rows(row_ids, EXPERTS))(expert_list)
        source = jnp.arange(EXPERTS, dtype=jnp.int32)[:, None]
        slot_index = (expert_list * (EXPERTS * CAP) + source * CAP + position).reshape(-1)
        grad_buffer = jnp.zeros((EXPERTS * EXPERTS * CAP, D_WIN), jnp.bfloat16).at[slot_index].set(grad_rows)
        hidden_buffer = jnp.zeros((EXPERTS * EXPERTS * CAP, F_WIN), jnp.bfloat16).at[slot_index].set(hidden_rows)
        grad_buffer = grad_buffer.reshape(EXPERTS, EXPERTS * CAP, D_WIN).astype(jnp.float32)
        hidden_buffer = hidden_buffer.reshape(EXPERTS, EXPERTS * CAP, F_WIN).astype(jnp.float32)
        grads = jnp.einsum('erf,erk->efk', hidden_buffer, grad_buffer)
        back = jnp.einsum('erk,efk->erf', grad_buffer, weight_full).astype(jnp.bfloat16)
        grad_hidden = back.reshape(EXPERTS * EXPERTS * CAP, F_WIN)[slot_index]
        merged = grads + error_in[replica].astype(jnp.float32)
        return (grad_hidden, merged)
    grad_hidden, merged = lax.map(one_replica, jnp.arange(N_DP, dtype=jnp.int32))
    grad_hidden = grad_hidden.reshape(ROWS, F_WIN)
    highest = lax.Precision.HIGHEST
    left_sum = jnp.einsum('defk,ekr->efr', merged, q_prev, precision=highest)
    gram = jnp.einsum('efr,efs->ers', left_sum, left_sum, precision=highest)
    chol = jnp.linalg.cholesky(gram)
    left_factor = lax.linalg.triangular_solve(chol, left_sum, left_side=False, lower=True, transpose_a=True)
    right_factor = jnp.einsum('defk,efr->ekr', merged, left_factor, precision=highest) / N_DP
    approx = jnp.einsum('efr,ekr->efk', left_factor, right_factor, precision=highest)
    error_out = (merged - approx[None]).astype(jnp.bfloat16)
    return (grad_hidden, left_factor, right_factor, error_out)
```

```python
import jax
import jax.numpy as jnp
from jax import lax
from jax.experimental import pallas as pl
from jax.experimental.pallas import tpu as pltpu
from jax.sharding import PartitionSpec as P

HIGHEST = lax.Precision.HIGHEST
F32 = jnp.float32
BF16 = jnp.bfloat16


def bits_of(size):
    return [1 << i for i in range(size.bit_length() - 1)]


def swap(value, axis, bit):
    size = lax.axis_size(axis)
    return lax.ppermute(value, axis, [(i, i ^ bit) for i in range(size)])


def shift(value, axis, step):
    size = lax.axis_size(axis)
    return lax.ppermute(value, axis, [(i, (i + step) % size) for i in range(size)])


def has_bit(bit):
    return (lax.axis_index("dp") & bit) != 0


def scatter_sum(value):
    for bit in bits_of(lax.axis_size("dp")):
        half = value.shape[0] // 2
        low, high = value[:half], value[half:]
        mine = has_bit(bit)
        sent = jnp.where(mine, low, high)
        kept = jnp.where(mine, high, low)
        value = kept + swap(sent, "dp", bit)
    return value


def gather_rows(value):
    for bit in reversed(bits_of(lax.axis_size("dp"))):
        other = swap(value, "dp", bit)
        mine = has_bit(bit)
        value = jnp.concatenate([jnp.where(mine, other, value), jnp.where(mine, value, other)], axis=0)
    return value


def own_block(value):
    size = lax.axis_size("dp")
    index = jnp.int32(0)
    for bit in bits_of(size):
        index = index * 2 + has_bit(bit).astype(jnp.int32)
    rows = value.shape[0] // size
    return lax.dynamic_slice_in_dim(value, index * rows, rows, 0)


def after(value, *others):
    return lax.optimization_barrier((value,) + others)[0]


def pack_kernel(experts, capacity, steps, rel_ref, grad_ref, hidden_ref, *out_refs):
    rows = grad_ref.shape[0]
    width = grad_ref.shape[1]
    rel = rel_ref[...]
    group = lax.broadcasted_iota(jnp.int32, (experts, rows), 0)
    onehot = (group == rel).astype(F32)
    before = (
        lax.broadcasted_iota(jnp.int32, (rows, rows), 0) < lax.broadcasted_iota(jnp.int32, (rows, rows), 1)
    ).astype(F32).astype(BF16)
    ranks = jnp.dot(onehot.astype(BF16), before, preferred_element_type=F32)
    rank = jnp.sum(ranks * onehot, axis=0, keepdims=True).astype(jnp.int32)
    slot = lax.broadcasted_iota(jnp.int32, (capacity, rows), 0)
    for step, out_ref in zip(steps, out_refs):
        target = jnp.where(rel == step, rank, -1)
        pick = (slot == target).astype(F32).astype(BF16)
        out_ref[:, :width] = jnp.dot(pick, grad_ref[...], preferred_element_type=F32).astype(BF16)
        out_ref[:, width:] = jnp.dot(pick, hidden_ref[...], preferred_element_type=F32).astype(BF16)


def pack(rel, grad_out, hidden_acts, capacity, steps):
    experts = lax.axis_size("expert")
    row_count, width = grad_out.shape
    total = width + hidden_acts.shape[1]
    return pl.pallas_call(
        lambda *refs: pack_kernel(experts, capacity, steps, *refs),
        out_shape=[jax.ShapeDtypeStruct((capacity, total), BF16) for _ in steps],
        name="pack_rows",
    )(rel.reshape(1, row_count), grad_out, hidden_acts)


def pad_lanes(value, lanes):
    return jnp.pad(value, ((0, 0), (0, lanes - value.shape[1])))


def shards(grad_out, hidden_acts, expert_ids, down_weight, error_in, q_prev):
    experts = lax.axis_size("expert")
    replicas = lax.axis_size("dp")
    place = lax.axis_index("expert")
    row_count, width = grad_out.shape
    hidden_width = hidden_acts.shape[1]
    capacity = 2 * row_count // experts
    rank = q_prev.shape[2]
    lanes = experts * rank
    rel = lax.rem(place - expert_ids + experts, experts)
    weight, q_own, error = down_weight[0], q_prev[0], error_in[0, 0]

    steps = list(range(1, experts))
    q_block = own_block(q_own)
    q_blocks = jnp.concatenate([q_block] + [shift(q_block, "expert", k) for k in steps], axis=1)
    weight_block = own_block(weight)
    weight_blocks = [shift(weight_block, "expert", k) for k in steps]
    packed_first = pack(rel, grad_out, hidden_acts, capacity, steps[:1])
    packed_rest = pack(rel, grad_out, hidden_acts, capacity, steps[1:])
    recv = [shift(packed_first[0], "expert", -1)]

    group = lax.broadcasted_iota(jnp.int32, (row_count, lanes), 1) // rank
    chosen = (group == rel[:, None]).astype(F32)
    error_f = error.astype(F32)
    grad_f = grad_out.astype(F32)
    hidden_f = hidden_acts.astype(F32)

    q_all = gather_rows(q_blocks)
    row_q = jnp.dot(grad_f, q_all, precision=HIGHEST) * chosen
    left_part = lax.dot_general(hidden_f, row_q, (((0,), (0,)), ((), ())), precision=HIGHEST)
    left_part = left_part + pad_lanes(jnp.dot(error_f, q_own, precision=HIGHEST), lanes)
    left_block = scatter_sum(left_part)
    left_recv = [shift(left_block, "expert", k) for k in steps]
    left_block_sum = left_block
    for k in steps:
        left_block_sum = left_block_sum + jnp.roll(left_recv[k - 1], k * rank, axis=1)
    left_sum = gather_rows(left_block_sum)

    packed_rest = [after(p, *left_recv) for p in packed_rest]
    recv += [shift(p, "expert", -k) for k, p in zip(steps[1:], packed_rest)]

    left_each = left_sum.reshape(hidden_width, experts, rank).transpose(1, 0, 2)
    gram = jnp.einsum("efr,efs->ers", left_each, left_each, precision=HIGHEST)
    chol = jnp.linalg.cholesky(gram)
    left_factors = lax.linalg.triangular_solve(chol, left_each, left_side=False, lower=True, transpose_a=True)
    left_own = left_factors[0]
    left_all = left_factors.transpose(1, 0, 2).reshape(hidden_width, lanes)

    row_l = jnp.dot(hidden_f, left_all, precision=HIGHEST) * chosen
    right_part = lax.dot_general(grad_f, row_l, (((0,), (0,)), ((), ())), precision=HIGHEST)
    right_part = right_part + pad_lanes(
        lax.dot_general(error_f, left_own, (((0,), (0,)), ((), ())), precision=HIGHEST), lanes
    )
    right_block = scatter_sum(right_part)
    right_recv = [shift(right_block[:, k * rank : (k + 1) * rank], "expert", -k) for k in steps]
    right_own = right_block[:, :rank]
    for r in right_recv:
        right_own = right_own + r
    right_factor = gather_rows(right_own) / replicas

    own_weight_block = weight_block
    blocks = jnp.concatenate([b[:, None] for b in weight_blocks], axis=1)
    blocks = after(blocks, left_sum)
    others = gather_rows(blocks)
    grad_hidden = lax.dot_general(grad_out, weight, (((1,), (1,)), ((), ())), preferred_element_type=F32)
    for k in steps:
        product = lax.dot_general(
            grad_out, others[:, k - 1], (((1,), (1,)), ((), ())), preferred_element_type=F32
        )
        grad_hidden = jnp.where((rel == k)[:, None], product, grad_hidden)
    grad_hidden = grad_hidden.astype(BF16)

    own_hidden = jnp.where((rel == 0)[:, None], hidden_acts, jnp.zeros((), BF16))
    rows_product = lambda h, g: lax.dot_general(h, g, (((0,), (0,)), ((), ())), preferred_element_type=F32)
    merged = error_f + rows_product(own_hidden, grad_out)
    for r in recv:
        merged = merged + rows_product(r[:, width:], r[:, :width])
    approx = lax.dot_general(left_own, right_factor, (((1,), (1,)), ((), ())), precision=HIGHEST)
    error_out = (merged - approx).astype(BF16)
    return (grad_hidden, left_own[None], right_factor[None], error_out[None, None])


def solution(mesh):
    placed = (
        P(("dp", "expert"), None),
        P(("dp", "expert"), None),
        P(("dp", "expert")),
        P("expert", None, None),
        P("dp", "expert", None, None),
        P("expert", None, None),
    )
    return jax.shard_map(
        shards,
        mesh=mesh,
        in_specs=placed,
        out_specs=(
            P(("dp", "expert"), None),
            P("expert", None, None),
            P("expert", None, None),
            P("dp", "expert", None, None),
        ),
        check_vma=False,
    )
```

```python
import jax
import jax.numpy as jnp
from jax import lax
from jax.experimental import pallas as pl
from jax.sharding import PartitionSpec as P


HIGHEST = lax.Precision.HIGHEST
F32 = jnp.float32
BF16 = jnp.bfloat16
LANES = 128


def dp_groups(size):
    bits = [1 << i for i in range(size.bit_length() - 1)]
    groups = [bits[:1]] + [bits[i : i + 2] for i in range(1, len(bits), 2)]
    return [g for g in groups if g]


def masks_of(group):
    return [sum(b for i, b in enumerate(group) if t >> i & 1) for t in range(1 << len(group))]


def flip(value, mask):
    size = lax.axis_size("dp")
    return lax.ppermute(value, "dp", [(i, i ^ mask) for i in range(size)])


def shift(value, step):
    size = lax.axis_size("expert")
    return lax.ppermute(value, "expert", [(i, (i + step) % size) for i in range(size)])


def place_in(group):
    index = lax.axis_index("dp")
    return sum(((index & bit) != 0).astype(jnp.int32) << i for i, bit in enumerate(group))


def scatter_sum(value):
    for group in dp_groups(lax.axis_size("dp")):
        masks = masks_of(group)
        rows = value.shape[0] // len(masks)
        place = place_in(group)
        block = lambda t: lax.dynamic_slice_in_dim(value, (place ^ t) * rows, rows, 0)
        total = block(0)
        for t in range(1, len(masks)):
            total = total + flip(block(t), masks[t])
        value = total
    return value


def gather_group(value, index, axis):
    group = dp_groups(lax.axis_size("dp"))[index]
    masks = masks_of(group)
    place = place_in(group)
    parts = [value] + [flip(value, masks[t]) for t in range(1, len(masks))]
    return jnp.concatenate([lax.select_n(place ^ t, *parts) if len(parts) > 2 else
                            jnp.where((place ^ t) == 0, parts[0], parts[1])
                            for t in range(len(masks))], axis=axis)


def gather_rows(value, axis=0):
    for i in reversed(range(len(dp_groups(lax.axis_size("dp"))))):
        value = gather_group(value, i, axis)
    return value


def own_block(value, count=None):
    index, size = jnp.int32(0), 1
    for group in dp_groups(lax.axis_size("dp"))[:count]:
        index = index * (1 << len(group)) + place_in(group)
        size <<= len(group)
    rows = value.shape[0] // size
    return lax.dynamic_slice_in_dim(value, index * rows, rows, 0)


def after(value, *others):
    return lax.optimization_barrier((value,) + others)[0]


def split3(value):
    high = value.astype(BF16)
    rest = value - high.astype(F32)
    mid = rest.astype(BF16)
    return high, mid, (rest - mid.astype(F32)).astype(BF16)


def dot3(exact, value, dims):
    out = None
    for term in reversed(split3(value)):
        part = lax.dot_general(exact, term, (dims, ((), ())), preferred_element_type=F32)
        out = part if out is None else out + part
    return out


ROWS_BY_ROWS = ((0,), (0,))
PLAIN = ((1,), (0,))


def rank_kernel(experts, steps, rel_ref, grad_ref, hidden_ref, rank_ref, *out_refs):
    rows = grad_ref.shape[0]
    rel = rel_ref[...]
    group = lax.broadcasted_iota(jnp.int32, (experts, rows), 0)
    onehot = (group == rel).astype(F32)
    before = (
        lax.broadcasted_iota(jnp.int32, (rows, rows), 0) < lax.broadcasted_iota(jnp.int32, (rows, rows), 1)
    ).astype(F32).astype(BF16)
    ranks = jnp.dot(onehot.astype(BF16), before, preferred_element_type=F32)
    rank = jnp.sum(ranks * onehot, axis=0, keepdims=True).astype(jnp.int32)
    rank_ref[...] = rank
    write_packed(rel, rank, steps, grad_ref, hidden_ref, out_refs)


def write_packed(rel, rank, steps, grad_ref, hidden_ref, out_refs):
    rows, width = grad_ref.shape
    for step, out_ref in zip(steps, out_refs):
        capacity = out_ref.shape[0]
        slot = lax.broadcasted_iota(jnp.int32, (capacity, rows), 0)
        target = jnp.where(rel == step, rank, -1)
        pick = (slot == target).astype(F32).astype(BF16)
        out_ref[:, :width] = jnp.dot(pick, grad_ref[...], preferred_element_type=F32).astype(BF16)
        out_ref[:, width:] = jnp.dot(pick, hidden_ref[...], preferred_element_type=F32).astype(BF16)


def pack_kernel(steps, rel_ref, rank_ref, grad_ref, hidden_ref, *out_refs):
    write_packed(rel_ref[...], rank_ref[...], steps, grad_ref, hidden_ref, out_refs)


def left_kernel(rank, grad_ref, hidden_ref, error_ref, q_ref, chosen_ref, out_ref):
    row_q = dot3(grad_ref[...], q_ref[...], PLAIN) * chosen_ref[...]
    own = dot3(error_ref[...], q_ref[:, :rank], PLAIN)
    out_ref[...] = dot3(hidden_ref[...], row_q, ROWS_BY_ROWS)
    out_ref[:, :rank] = out_ref[:, :rank] + own


def orthonormal(left, rank):
    chunk = left.shape[1]
    each = chunk // rank
    full = lax.dot_general(
        left, left, (ROWS_BY_ROWS, ((), ())), precision=HIGHEST, preferred_element_type=F32
    )
    lane = lax.broadcasted_iota(jnp.int32, (rank, chunk), 1)
    row = lax.broadcasted_iota(jnp.int32, (rank, chunk), 0)
    inner = lane % rank
    base = lane - inner
    gram = jnp.zeros((rank, chunk), F32)
    for e in range(each):
        gram = jnp.where(base == e * rank, full[e * rank : (e + 1) * rank, :], gram)
    inverse = (inner == row).astype(F32)
    scale = jnp.zeros((rank, chunk), F32)
    for j in range(rank):
        column = jnp.take_along_axis(gram, base + j, axis=1)
        pivot = 1.0 / column[j : j + 1]
        factor = jnp.where(row > j, column * pivot, 0.0)
        scale = jnp.where(row == j, column[j : j + 1], scale)
        gram, inverse = gram - factor * gram[j : j + 1], inverse - factor * inverse[j : j + 1]
    inverse = inverse * lax.rsqrt(scale)
    wide = jnp.concatenate([inverse] * each, axis=0)
    wide_row = lax.broadcasted_iota(jnp.int32, (chunk, chunk), 0)
    wide_lane = lax.broadcasted_iota(jnp.int32, (chunk, chunk), 1)
    wide = jnp.where(wide_row // rank == wide_lane // rank, wide, 0.0)
    return lax.dot_general(left, wide, (((1,), (1,)), ((), ())), precision=HIGHEST, preferred_element_type=F32)


def right_kernel(rank, left_ref, grad_ref, hidden_ref, error_ref, chosen_ref, own_ref, out_ref):
    lanes = left_ref.shape[1]
    chunk = min(lanes, LANES)
    for start in range(0, lanes, chunk):
        part = slice(start, start + chunk)
        factors = orthonormal(left_ref[:, part], rank)
        row_l = dot3(hidden_ref[...], factors, PLAIN) * chosen_ref[:, part]
        out_ref[:, part] = dot3(grad_ref[...], row_l, ROWS_BY_ROWS)
        if start == 0:
            own_ref[...] = factors[:, :rank]
            own = dot3(error_ref[...], factors[:, :rank], ROWS_BY_ROWS)
            out_ref[:, :rank] = out_ref[:, :rank] + own


def call(kernel, shapes, *args):
    return pl.pallas_call(kernel, out_shape=[jax.ShapeDtypeStruct(s, t) for s, t in shapes])(*args)


def phases(experts):
    steps = list(range(1, experts))
    count = len(steps)
    cuts = [0, (count + 2) // 3, (2 * count + 2) // 3, count]
    return [steps[a:b] for a, b in zip(cuts, cuts[1:])]


def shards(grad_out, hidden_acts, expert_ids, down_weight, error_in, q_prev):
    experts = lax.axis_size("expert")
    replicas = lax.axis_size("dp")
    place = lax.axis_index("expert")
    row_count, width = grad_out.shape
    hidden_width = hidden_acts.shape[1]
    capacity = 2 * row_count // experts
    rank = q_prev.shape[2]
    lanes = experts * rank
    total = width + hidden_width
    rel = lax.rem(place - expert_ids + experts, experts)
    rel_row = rel.reshape(1, row_count)
    weight, q_own, error = down_weight[0], q_prev[0], error_in[0, 0]
    chosen = (lax.broadcasted_iota(jnp.int32, (row_count, lanes), 1) // rank == rel[:, None]).astype(F32)

    steps = list(range(1, experts))
    parts = phases(experts)
    send_rows = lambda packed, ks: [shift(p, -k) for k, p in zip(ks, packed)]
    q_block = own_block(q_own, 1)
    q_blocks = [q_block] + [shift(q_block, k) for k in steps]
    row_rank, *packed = call(
        lambda *refs: rank_kernel(experts, parts[0], *refs),
        [((1, row_count), jnp.int32)] + [((capacity, total), BF16) for _ in parts[0]],
        rel_row, grad_out, hidden_acts,
    )
    recv = send_rows(packed, parts[0])

    q_all = gather_group(jnp.concatenate(q_blocks, axis=1), 0, 0)
    (left_part,) = call(
        lambda *refs: left_kernel(rank, *refs), [((hidden_width, lanes), F32)],
        grad_out, hidden_acts, error, q_all, chosen,
    )
    left_block = scatter_sum(left_part)
    left_sum = left_block
    for k in steps:
        left_sum = left_sum + jnp.roll(shift(left_block, k), k * rank, axis=1)

    weight_block = own_block(weight)
    weight_blocks = jnp.stack([shift(weight_block, k) for k in steps])
    rest = parts[1] + parts[2]
    packed = call(
        lambda *refs: pack_kernel(rest, *refs), [((capacity, total), BF16) for _ in rest],
        rel_row, after(row_rank, left_block), grad_out, hidden_acts,
    )
    recv += send_rows(packed, rest)

    left_sum = gather_rows(left_sum)
    left_own, right_part = call(
        lambda *refs: right_kernel(rank, *refs),
        [((hidden_width, rank), F32), ((width, lanes), F32)],
        left_sum, grad_out, hidden_acts, error, chosen,
    )
    right_block = scatter_sum(right_part)
    right_own = right_block[:, :rank]
    for k in steps:
        right_own = right_own + shift(right_block[:, k * rank : (k + 1) * rank], -k)
    right_factor = gather_rows(right_own) / replicas

    others = gather_rows(weight_blocks, 1)
    rows_back = lambda w: lax.dot_general(grad_out, w, (((1,), (1,)), ((), ())), preferred_element_type=F32)
    grad_hidden = rows_back(weight)
    for k in steps:
        grad_hidden = jnp.where((rel == k)[:, None], rows_back(others[k - 1]), grad_hidden)
    grad_hidden = grad_hidden.astype(BF16)

    own_hidden = jnp.where((rel == 0)[:, None], hidden_acts, jnp.zeros((), BF16))
    rows_product = lambda h, g: lax.dot_general(h, g, (ROWS_BY_ROWS, ((), ())), preferred_element_type=F32)
    merged = error.astype(F32) + rows_product(own_hidden, grad_out)
    for r in recv:
        merged = merged + rows_product(r[:, width:], r[:, :width])
    approx = lax.dot_general(left_own, right_factor, (((1,), (1,)), ((), ())), precision=HIGHEST)
    error_out = (merged - approx).astype(BF16)
    return (grad_hidden, left_own[None], right_factor[None], error_out[None, None])


def solution(mesh):
    placed = (
        P(("dp", "expert"), None),
        P(("dp", "expert"), None),
        P(("dp", "expert")),
        P("expert", None, None),
        P("dp", "expert", None, None),
        P("expert", None, None),
    )
    return jax.shard_map(
        shards,
        mesh=mesh,
        in_specs=placed,
        out_specs=(
            P(("dp", "expert"), None),
            P("expert", None, None),
            P("expert", None, None),
            P("dp", "expert", None, None),
        ),
        check_vma=False,
    )
```
